32 devices in a mesh: gx: 4 (over y, x), gy: 4 (over z), gz: 2 (over core).
Axes of the slice: x: 2, y: 2, z: 4, core: 2. Of those that a mesh axis runs over, the one named last changes fastest.
Arguments:
- right_side: float32 [5, 512, 8, 128], P(None, ('gx', 'gy', 'gz')), may hold values from -6 to 6
- diag_inverse: bfloat16 [5, 512, 128, 128], P(None, ('gx', 'gy', 'gz')), may hold values from -0.5 to 0.5
- off_blocks: bfloat16 [4, 1024, 128, 128], P(None, ('gx', 'gy', 'gz')), may hold values from -0.375 to 0.375
- live_counts: int32 [5, 32], P(None, ('gx', 'gy', 'gz')), may hold values from 1 to 16, as said below
- source_slot: int32 [4, 1024], P(None, ('gx', 'gy', 'gz')), may hold values from 0 to 15, as said below
- target_owner: int32 [4, 1024], P(None, ('gx', 'gy', 'gz')), may hold values from 0 to 31, as said below
- target_block: int32 [4, 1024], P(None, ('gx', 'gy', 'gz')), may hold values from 16 to 79, as said below
Outputs:
- solution: float32 [5, 512, 8, 128], P(None, ('gx', 'gy', 'gz'))
The draws below stay inside these ranges and needn't reach their ends.
Inputs may be any that keep to these rules, and one draw needn't show every extreme that they name: `live_counts`: slots at or past a device's count in a level are empty; in every level some device has all 16 slots live. `source_slot`: names a live slot of the issuing device in the same level. `target_owner`: in every level, each device's records go exactly 2 each to 16 distinct owners and none to the others. `target_block`: the level part is later than the record's own level, and the slot is live at the owner in that level.
All inputs are finite; a program needn't handle non-finite values.
Results may differ from the reference program's by a relative error of at most 0.013.
Values sent between devices are 32-bit elements; how exact they have to be, the bound alone decides.
A program may use at most 64 MiB of HBM per device.

```python
import jax
import jax.numpy as jnp
from jax import lax

B = 128
R = 8
LEVELS = 5
S = 16
CAP = 2
OWNERS = 32
RECS = 32
NBLK = 512


def routing(key):
    base = jax.random.fold_in(key, 7)
    key_count, key_full, key_perm, key_src, key_level, key_slot = jax.random.split(base, 6)
    counts = jax.random.randint(key_count, (LEVELS, OWNERS), 1, S + 1)
    full_owner = jax.random.randint(key_full, (LEVELS,), 0, OWNERS)
    counts = counts.at[jnp.arange(LEVELS), full_owner].set(S)

    def one_list(sub_key):
        first_key, second_key = jax.random.split(sub_key)
        chosen = jax.random.permutation(first_key, OWNERS)[:OWNERS // 2].astype(jnp.int32)
        whole_list = jnp.repeat(chosen, CAP)
        return whole_list[jax.random.permutation(second_key, RECS)]
    list_keys = jax.random.split(key_perm, (LEVELS - 1) * OWNERS)
    owners = jax.vmap(one_list)(list_keys).reshape(LEVELS - 1, OWNERS, RECS)
    shape = (LEVELS - 1, OWNERS, RECS)
    sources = jax.random.randint(key_src, shape, 0, counts[:-1, :, None])
    lowest = (jnp.arange(LEVELS - 1, dtype=jnp.int32) + 1)[:, None, None]
    target_level = jax.random.randint(key_level, shape, lowest, LEVELS)
    target_slot = jax.random.randint(key_slot, shape, 0, counts[target_level, owners])
    blocks = target_level * S + target_slot
    flat = (LEVELS - 1, OWNERS * RECS)
    return (counts.astype(jnp.int32), sources.reshape(flat).astype(jnp.int32), owners.reshape(flat).astype(jnp.int32), blocks.reshape(flat).astype(jnp.int32))


def draw_live_counts(key, part):
    return routing(key)[0]


def draw_source_slot(key, part):
    return routing(key)[1]


def draw_target_owner(key, part):
    return routing(key)[2]


def draw_target_block(key, part):
    return routing(key)[3]


def block_scale(stream_key, shape, cuts, low, high):
    def one(position, shards_of):
        steps = jax.random.uniform(jax.random.fold_in(jax.random.fold_in(stream_key, 6), position), (shards_of,), jnp.float32, low / len(cuts), high / len(cuts))
        return jnp.repeat(jnp.exp(steps), shape[position] // shards_of).reshape((-1,) + (1,) * (len(shape) - position - 1))

    gain = one(*cuts[0])
    for cut in cuts[1:]:
        gain = gain * one(*cut)
    return gain


def scatter_about(own_key, shape, scale, bound, cuts=(), kind=jnp.bfloat16):
    drawn = scale * jax.random.normal(own_key, shape, jnp.float32)
    if cuts:
        drawn = drawn * block_scale(own_key, shape, cuts, -0.22, 0.18)
    return jnp.clip(drawn, -bound, bound).astype(kind)


def setup_inputs(seed: int = 0) -> dict:
    streams_of = jax.random.split(jax.random.key(seed), 8)
    right_side = scatter_about(streams_of[0], (LEVELS, NBLK, R, B), 1.0, 6.0, ((1, 32),), jnp.float32)
    diag_inverse = scatter_about(streams_of[1], (LEVELS, NBLK, B, B), B ** -0.5, 0.5, ((1, 32),))
    off_blocks = scatter_about(streams_of[2], (LEVELS - 1, OWNERS * RECS, B, B), (2 * B) ** -0.5, 0.375, ((1, 32),))
    live_counts = draw_live_counts(jax.random.fold_in(streams_of[7], 71), 0)
    source_slot = draw_source_slot(jax.random.fold_in(streams_of[7], 71), 0)
    target_owner = draw_target_owner(jax.random.fold_in(streams_of[7], 71), 0)
    target_block = draw_target_block(jax.random.fold_in(streams_of[7], 71), 0)
    return {"right_side": right_side, "diag_inverse": diag_inverse, "off_blocks": off_blocks, "live_counts": live_counts, "source_slot": source_slot, "target_owner": target_owner, "target_block": target_block}


def reference(right_side, diag_inverse, off_blocks, live_counts, source_slot, target_owner, target_block):
    accumulated = jnp.zeros((LEVELS * NBLK, R, B), jnp.float32)
    slot_ids = jnp.arange(S, dtype=jnp.int32)
    solved_all = []
    for level_at in range(LEVELS):
        live = (slot_ids[None, :] < live_counts[level_at][:, None]).reshape(NBLK)
        pending = accumulated[level_at * NBLK:(level_at + 1) * NBLK]
        work_rows = (right_side[level_at] - pending).astype(jnp.bfloat16)
        solved = jnp.einsum('nrb,nbc->nrc', work_rows.astype(jnp.float32), diag_inverse[level_at].astype(jnp.float32))
        solved = jnp.where(live[:, None, None], solved, jnp.float32(0.0))
        solved_all.append(solved)
        if level_at + 1 < LEVELS:
            rounded = solved.astype(jnp.bfloat16).reshape(OWNERS, S, R, B)
            blocks = off_blocks[level_at].reshape(OWNERS, RECS, B, B)
            slot_lists = source_slot[level_at].reshape(OWNERS, RECS)

            def per_owner(items):
                owner_rows, owner_blocks, owner_slots = items
                picked = owner_rows[owner_slots]
                return jnp.einsum('krb,kbc->krc', picked.astype(jnp.float32), owner_blocks.astype(jnp.float32))

            contributions = lax.map(per_owner, (rounded, blocks, slot_lists)).reshape(OWNERS * RECS, R, B)
            owner_ids = target_owner[level_at].astype(jnp.int32)
            targets = target_block[level_at].astype(jnp.int32)
            row_ids = (targets // S) * NBLK + owner_ids * S + targets % S
            accumulated = accumulated.at[row_ids].add(contributions)
    return jnp.stack(solved_all)
```

```python
import functools

import jax
import jax.numpy as jnp
from jax import lax
from jax.experimental import pallas as pl
from jax.experimental.pallas import tpu as pltpu
from jax.sharding import PartitionSpec as P

CAP = 2
AXES = ("gx", "gy", "gz")
MESH = pl.DeviceIdType.MESH


def kernel(
    sizes,
    live_ref,
    source_ref,
    record_ref,
    labels_ref,
    right_hbm,
    diag_hbm,
    off_hbm,
    out_hbm,
    work_ref,
    diag_ref,
    off_ref,
    solved_ref,
    made_ref,
    outgoing_ref,
    arrived_ref,
    names_ref,
    load_sem,
    out_sem,
    send_sem,
    recv_sem,
    name_send_sem,
    name_recv_sem,
):
    nx, ny, nz = sizes
    devices = nx * ny * nz
    levels, slots = diag_ref.shape[:2]
    records = off_ref.shape[1]
    rhs = solved_ref.shape[-2]
    pack = CAP * rhs
    level_rows = slots * rhs
    arrivals = devices * CAP
    me = (lax.axis_index("gx") * ny + lax.axis_index("gy")) * nz + lax.axis_index("gz")

    def place(device):
        return (device // (ny * nz), (device // nz) % ny, device % nz)

    def partner(step):
        return lax.rem(me + step, devices)

    right_load = pltpu.make_async_copy(right_hbm, work_ref, load_sem.at[0])
    diag_loads = [
        pltpu.make_async_copy(diag_hbm.at[at], diag_ref.at[at], load_sem.at[1 + at])
        for at in range(levels)
    ]
    off_loads = [
        pltpu.make_async_copy(off_hbm.at[at], off_ref.at[at], load_sem.at[1 + levels + at])
        for at in range(levels - 1)
    ]
    right_load.start()
    for at in range(levels):
        diag_loads[at].start()
        if at < levels - 1:
            off_loads[at].start()

    barrier = pltpu.get_barrier_semaphore()

    @pl.loop(1, devices)
    def _(step):
        pl.semaphore_signal(barrier, inc=1, device_id=place(partner(step)), device_id_type=MESH)

    pl.semaphore_wait(barrier, devices - 1)

    @pl.loop(1, devices)
    def _(step):
        other = partner(step)
        pltpu.make_async_remote_copy(
            src_ref=labels_ref.at[other],
            dst_ref=names_ref.at[me],
            send_sem=name_send_sem,
            recv_sem=name_recv_sem,
            device_id=place(other),
            device_id_type=MESH,
        ).start()

    names_ref[me] = labels_ref[me]
    right_load.wait()

    names = None
    for at in range(levels):
        diag_loads[at].wait()
        count = live_ref[at, 0]
        for slot in range(slots):
            row = (at * slots + slot) * rhs
            work = work_ref[row : row + rhs, :].astype(jnp.bfloat16)
            solved = jnp.dot(work, diag_ref[at, slot], preferred_element_type=jnp.float32)
            solved_ref[at, slot] = jnp.where(slot < count, solved, jnp.float32(0.0))
        pltpu.make_async_copy(solved_ref.at[at], out_hbm.at[at], out_sem.at[at]).start()
        if at == levels - 1:
            break
        off_loads[at].wait()

        def make(record, carry, at=at):
            picked = solved_ref[at, source_ref[at, record]].astype(jnp.bfloat16)
            made_ref[record] = jnp.dot(
                picked, off_ref[at, record], preferred_element_type=jnp.float32
            )
            return carry

        lax.fori_loop(0, records, make, 0, unroll=True)

        def send(step, carry, at=at):
            other = partner(step)
            for copy_at in range(CAP):
                outgoing_ref[at, pl.ds(other * pack + copy_at * rhs, rhs), :] = made_ref[
                    record_ref[at, other * CAP + copy_at]
                ]
            pltpu.make_async_remote_copy(
                src_ref=outgoing_ref.at[at, pl.ds(other * pack, pack)],
                dst_ref=arrived_ref.at[at, pl.ds(me * pack, pack)],
                send_sem=send_sem.at[at],
                recv_sem=recv_sem.at[at],
                device_id=place(other),
                device_id_type=MESH,
            ).start()
            return carry

        lax.fori_loop(1, devices, send, 0)
        for copy_at in range(CAP):
            arrived_ref[at, pl.ds(me * pack + copy_at * rhs, rhs), :] = made_ref[
                record_ref[at, me * CAP + copy_at]
            ]

        if at == 0:
            pltpu.make_async_copy(
                names_ref.at[pl.ds(0, devices - 1)],
                names_ref.at[pl.ds(0, devices - 1)],
                name_recv_sem,
            ).wait()
            names = jnp.sum(names_ref[...], axis=0)

        later_rows = (levels - 1 - at) * slots
        ids = lax.broadcasted_iota(jnp.int32, (later_rows, arrivals), 0) + (
            (at + 1) * slots + 1
        )
        hit = (ids == names[at : at + 1, :arrivals]).astype(jnp.float32).astype(jnp.bfloat16)
        placer = jnp.concatenate([hit, hit], axis=1)

        incoming = arrived_ref.at[at, pl.ds(0, (devices - 1) * pack)]
        pltpu.make_async_copy(incoming, incoming, recv_sem.at[at]).wait()
        for r in range(rhs):
            row = arrived_ref[at, pl.ds(r, arrivals, stride=rhs), :]
            high = row.astype(jnp.bfloat16)
            low = (row - high.astype(jnp.float32)).astype(jnp.bfloat16)
            total = jnp.dot(
                placer,
                jnp.concatenate([high, low], axis=0),
                preferred_element_type=jnp.float32,
            )
            where = pl.ds((at + 1) * level_rows + r, later_rows, stride=rhs)
            work_ref[where, :] = work_ref[where, :] - total

    for at in range(levels):
        pltpu.make_async_copy(solved_ref.at[at], out_hbm.at[at], out_sem.at[at]).wait()
    name_part = labels_ref.at[pl.ds(0, devices - 1)]
    pltpu.make_async_copy(name_part, name_part, name_send_sem).wait()
    for at in range(levels - 1):
        part = outgoing_ref.at[at, pl.ds(0, (devices - 1) * pack)]
        pltpu.make_async_copy(part, part, send_sem.at[at]).wait()


def shards(
    sizes,
    right_side,
    diag_inverse,
    off_blocks,
    live_counts,
    source_slot,
    target_owner,
    target_block,
):
    levels, slots, rhs, width = right_side.shape
    records = off_blocks.shape[1]
    devices = sizes[0] * sizes[1] * sizes[2]
    arrivals = devices * CAP
    lanes = -(-arrivals // 128) * 128
    me = (lax.axis_index("gx") * sizes[1] + lax.axis_index("gy")) * sizes[2] + lax.axis_index(
        "gz"
    )

    record_ids = jnp.arange(records, dtype=jnp.int32)
    same = (target_owner[:, :, None] == target_owner[:, None, :]) & (
        record_ids[None, None, :] < record_ids[None, :, None]
    )
    slot_of = target_owner * CAP + jnp.sum(same.astype(jnp.int32), axis=2)
    packer = slot_of[:, None, :] == jnp.arange(arrivals, dtype=jnp.int32)[None, :, None]
    record_at = jnp.sum(jnp.where(packer, record_ids[None, None, :], 0), axis=2)
    label = jnp.sum(jnp.where(packer, target_block[:, None, :] + 1, 0), axis=2)
    label = label.reshape(levels - 1, devices, CAP).transpose(1, 0, 2)
    lane_ids = jnp.arange(lanes, dtype=jnp.int32)
    labels = jnp.zeros((devices, levels - 1, lanes), jnp.int32)
    for copy_at in range(CAP):
        labels = jnp.where(
            lane_ids[None, None, :] == me * CAP + copy_at, label[:, :, copy_at : copy_at + 1], labels
        )

    smem = pl.BlockSpec(memory_space=pltpu.SMEM)
    vmem = pl.BlockSpec(memory_space=pltpu.VMEM)
    anywhere = pl.BlockSpec(memory_space=pl.ANY)
    return pl.pallas_call(
        functools.partial(kernel, sizes),
        out_shape=jax.ShapeDtypeStruct((levels, slots, rhs, width), jnp.float32),
        in_specs=[smem, smem, smem, vmem, anywhere, anywhere, anywhere],
        out_specs=anywhere,
        scratch_shapes=[
            pltpu.VMEM((levels * slots * rhs, width), jnp.float32),
            pltpu.VMEM(diag_inverse.shape, diag_inverse.dtype),
            pltpu.VMEM(off_blocks.shape, off_blocks.dtype),
            pltpu.VMEM((levels, slots, rhs, width), jnp.float32),
            pltpu.VMEM((records, rhs, width), jnp.float32),
            pltpu.VMEM((levels - 1, arrivals * rhs, width), jnp.float32),
            pltpu.VMEM((levels - 1, arrivals * rhs, width), jnp.float32),
            pltpu.VMEM((devices, levels - 1, lanes), jnp.int32),
            pltpu.SemaphoreType.DMA((2 * levels,)),
            pltpu.SemaphoreType.DMA((levels,)),
            pltpu.SemaphoreType.DMA((levels - 1,)),
            pltpu.SemaphoreType.DMA((levels - 1,)),
            pltpu.SemaphoreType.DMA,
            pltpu.SemaphoreType.DMA,
        ],
        compiler_params=pltpu.CompilerParams(
            collective_id=0, has_side_effects=True, vmem_limit_bytes=60 * 1024 * 1024
        ),
    )(
        live_counts,
        source_slot,
        record_at,
        labels,
        right_side.reshape(levels * slots * rhs, width),
        diag_inverse,
        off_blocks,
    )


def solution(mesh):
    sizes = tuple(mesh.shape[axis] for axis in AXES)
    in_specs = (
        P(None, AXES, None, None),
        P(None, AXES, None, None),
        P(None, AXES, None, None),
        P(None, AXES),
        P(None, AXES),
        P(None, AXES),
        P(None, AXES),
    )
    return jax.shard_map(
        functools.partial(shards, sizes),
        mesh=mesh,
        in_specs=in_specs,
        out_specs=P(None, AXES, None, None),
        check_vma=False,
    )
```

```python
import functools

import jax
import jax.numpy as jnp
from jax import lax
from jax.experimental import pallas as pl
from jax.experimental.pallas import tpu as pltpu
from jax.sharding import PartitionSpec as P

CAP = 2
GROUP = 8
AXES = ("gx", "gy", "gz")
MESH = pl.DeviceIdType.MESH


def kernel(
    sizes,
    live_ref,
    source_ref,
    owner_ref,
    block_ref,
    right_hbm,
    diag_hbm,
    off_hbm,
    out_hbm,
    work_ref,
    diag_ref,
    off_refs,
    solved_ref,
    outgoing_ref,
    arrived_ref,
    names_out_ref,
    names_ref,
    record_vmem,
    record_ref,
    load_sem,
    out_sem,
    record_sem,
    send_sem,
    recv_sem,
    name_send_sem,
    name_recv_sem,
):
    nx, ny, nz = sizes
    devices = nx * ny * nz
    plane = nx * nz
    levels, slots = diag_ref.shape[:2]
    records = off_refs[0].shape[0]
    rhs = solved_ref.shape[-2]
    pack = CAP * rhs
    level_rows = slots * rhs
    lanes = names_ref.shape[-1]
    mx, my, mz = (lax.axis_index(axis) for axis in AXES)
    me = (mx * ny + my) * nz + mz

    def partner(index):
        at = index // plane
        down = ny - 1 - at
        down = down - jnp.where(down > my, 0, 1)
        up = at + jnp.where(at < my, 0, 1)
        oy = jnp.where(at == ny - 1, my, jnp.where(2 * my < ny, down, up))
        rest = lax.rem(index, plane) + 1
        ox = lax.rem(mx + rest // nz, nx)
        oz = lax.rem(mz + lax.rem(rest, nz), nz)
        return (ox * ny + oy) * nz + oz, (ox, oy, oz)

    right_load = pltpu.make_async_copy(right_hbm, work_ref, load_sem.at[0])
    diag_loads = [
        pltpu.make_async_copy(diag_hbm.at[at], diag_ref.at[at], load_sem.at[1 + at])
        for at in range(levels)
    ]
    off_loads = [
        pltpu.make_async_copy(off_hbm.at[at], off_refs[at], load_sem.at[1 + levels + at])
        for at in range(levels - 1)
    ]
    barrier = pltpu.get_barrier_semaphore()

    @pl.loop(0, devices - 1)
    def _(index):
        pl.semaphore_signal(barrier, inc=1, device_id=partner(index)[1], device_id_type=MESH)

    right_load.start()
    for at in range(levels):
        diag_loads[at].start()
        if at < levels - 1:
            off_loads[at].start()

    owner_ids = lax.broadcasted_iota(jnp.int32, (devices, records), 0)
    record_ids = lax.broadcasted_iota(jnp.int32, (devices, records), 1)
    lane_ids = lax.broadcasted_iota(jnp.int32, (devices, lanes), 1)
    told = jnp.zeros((devices, lanes), jnp.float32)
    index = jnp.zeros((devices, lanes), jnp.int32)
    for at in range(levels - 1):
        hits = owner_ids == owner_ref[at : at + 1, :]
        block_row = (block_ref[at : at + 1, :] + 1).astype(jnp.float32)
        first = jnp.min(jnp.where(hits, record_ids, records - 1), axis=1, keepdims=True)
        last = jnp.max(jnp.where(hits, record_ids, 0), axis=1, keepdims=True)
        for copy_at, record in enumerate((first, last)):
            chosen = jnp.where(hits & (record_ids == record), block_row, 0.0)
            label = jnp.sum(chosen, axis=1, keepdims=True)
            told = jnp.where(lane_ids == at * CAP + copy_at, label, told)
            index = jnp.where(lane_ids == at * CAP + copy_at, record, index)
    record_vmem[...] = index
    names_out_ref[...] = told.reshape(devices, 1, lanes)
    names_ref[pl.ds(me, 1)] = names_out_ref[pl.ds(me, 1)]
    record_copy = pltpu.make_async_copy(record_vmem, record_ref, record_sem)
    record_copy.start()

    def solve(at):
        diag_loads[at].wait()
        count = live_ref[0, at]
        for slot in range(slots):
            row = (at * slots + slot) * rhs
            work = work_ref[row : row + rhs, :].astype(jnp.bfloat16)
            solved = jnp.dot(work, diag_ref[at, slot], preferred_element_type=jnp.float32)
            solved_ref[at, slot] = jnp.where(slot < count, solved, jnp.float32(0.0))
        pltpu.make_async_copy(solved_ref.at[at], out_hbm.at[at], out_sem.at[at]).start()

    def make(at, other, target_ref, base):
        for copy_at in range(CAP):
            record = record_ref[other, at * CAP + copy_at]
            picked = solved_ref[at, source_ref[at, record]].astype(jnp.bfloat16)
            target_ref[at, pl.ds(base + copy_at * rhs, rhs), :] = jnp.dot(
                picked, off_refs[at][record], preferred_element_type=jnp.float32
            )

    def make_out(at, index):
        other, _ = partner(index)
        make(at, other, outgoing_ref, other * pack)

    def send(at, index):
        other, where = partner(index)
        pltpu.make_async_remote_copy(
            src_ref=outgoing_ref.at[at, pl.ds(other * pack, pack)],
            dst_ref=arrived_ref.at[at, pl.ds(me * pack, pack)],
            send_sem=send_sem.at[at],
            recv_sem=recv_sem.at[at],
            device_id=where,
            device_id_type=MESH,
        ).start()

    def send_all(at):
        groups = devices // GROUP

        @pl.loop(0, groups - 1)
        def _(group):
            for item in range(GROUP):
                make_out(at, group * GROUP + item)
            for item in range(GROUP):
                send(at, group * GROUP + item)

        for index in range(devices - GROUP, devices - 1):
            make_out(at, index)
        for index in range(devices - GROUP, devices - 1):
            send(at, index)
        make(at, me, arrived_ref, me * pack)

    def gather_in(at, names, first, count):
        ids = lax.broadcasted_iota(jnp.int32, (count * slots, devices), 0) + (first * slots + 1)
        hits = [
            (ids == names[at * CAP + copy_at : at * CAP + copy_at + 1, :])
            .astype(jnp.float32)
            .astype(jnp.bfloat16)
            for copy_at in range(CAP)
        ]
        placer = jnp.concatenate(hits + hits, axis=1)
        for r in range(rhs):
            rows = [
                arrived_ref[at, pl.ds(copy_at * rhs + r, devices, stride=pack), :]
                for copy_at in range(CAP)
            ]
            high = [row.astype(jnp.bfloat16) for row in rows]
            low = [
                (row - top.astype(jnp.float32)).astype(jnp.bfloat16)
                for row, top in zip(rows, high)
            ]
            total = jnp.dot(
                placer,
                jnp.concatenate(high + low, axis=0),
                preferred_element_type=jnp.float32,
            )
            where = pl.ds(first * level_rows + r, count * slots, stride=rhs)
            work_ref[where, :] = work_ref[where, :] - total

    right_load.wait()
    solve(0)
    record_copy.wait()
    off_loads[0].wait()
    pl.semaphore_wait(barrier, devices - 1)

    @pl.loop(0, devices - 1)
    def _(index):
        other, where = partner(index)
        pltpu.make_async_remote_copy(
            src_ref=names_out_ref.at[pl.ds(other, 1)],
            dst_ref=names_ref.at[pl.ds(me, 1)],
            send_sem=name_send_sem,
            recv_sem=name_recv_sem,
            device_id=where,
            device_id_type=MESH,
        ).start()

    send_all(0)
    name_part = names_ref.at[pl.ds(0, devices - 1)]
    pltpu.make_async_copy(name_part, name_part, name_recv_sem).wait()
    wanted = -(-(levels - 1) * CAP // 8) * 8
    pick = (
        lax.broadcasted_iota(jnp.int32, (wanted, lanes), 0)
        == lax.broadcasted_iota(jnp.int32, (wanted, lanes), 1)
    ).astype(jnp.float32)
    names = lax.dot_general(
        pick,
        names_ref[...].reshape(devices, lanes),
        (((1,), (1,)), ((), ())),
        preferred_element_type=jnp.float32,
        precision=lax.Precision.HIGHEST,
    ).astype(jnp.int32)

    for at in range(1, levels):
        incoming = arrived_ref.at[at - 1, pl.ds(0, (devices - 1) * pack)]
        pltpu.make_async_copy(incoming, incoming, recv_sem.at[at - 1]).wait()
        gather_in(at - 1, names, at, 1)
        solve(at)
        if at < levels - 1:
            off_loads[at].wait()
            send_all(at)
            gather_in(at - 1, names, at + 1, levels - 1 - at)

    for at in range(levels):
        pltpu.make_async_copy(solved_ref.at[at], out_hbm.at[at], out_sem.at[at]).wait()
    name_part = names_out_ref.at[pl.ds(0, devices - 1)]
    pltpu.make_async_copy(name_part, name_part, name_send_sem).wait()
    for at in range(levels - 1):
        part = outgoing_ref.at[at, pl.ds(0, (devices - 1) * pack)]
        pltpu.make_async_copy(part, part, send_sem.at[at]).wait()


def shards(
    sizes,
    right_side,
    diag_inverse,
    off_blocks,
    live_counts,
    source_slot,
    target_owner,
    target_block,
):
    levels, slots, rhs, width = right_side.shape
    records = off_blocks.shape[1]
    devices = sizes[0] * sizes[1] * sizes[2]
    arrivals = devices * CAP
    lanes = 128
    smem = pl.BlockSpec(memory_space=pltpu.SMEM)
    vmem = pl.BlockSpec(memory_space=pltpu.VMEM)
    anywhere = pl.BlockSpec(memory_space=pl.ANY)
    return pl.pallas_call(
        functools.partial(kernel, sizes),
        out_shape=jax.ShapeDtypeStruct((levels, slots, rhs, width), jnp.float32),
        in_specs=[smem, smem, vmem, vmem, anywhere, anywhere, anywhere],
        out_specs=anywhere,
        scratch_shapes=[
            pltpu.VMEM((levels * slots * rhs, width), jnp.float32),
            pltpu.VMEM(diag_inverse.shape, diag_inverse.dtype),
            tuple(
                pltpu.VMEM(off_blocks.shape[1:], off_blocks.dtype) for _ in range(levels - 1)
            ),
            pltpu.VMEM((levels, slots, rhs, width), jnp.float32),
            pltpu.VMEM((levels - 1, arrivals * rhs, width), jnp.float32),
            pltpu.VMEM((levels - 1, arrivals * rhs, width), jnp.float32),
            pltpu.VMEM((devices, 1, lanes), jnp.float32),
            pltpu.VMEM((devices, 1, lanes), jnp.float32),
            pltpu.VMEM((devices, lanes), jnp.int32),
            pltpu.SMEM((devices, lanes), jnp.int32),
            pltpu.SemaphoreType.DMA((2 * levels,)),
            pltpu.SemaphoreType.DMA((levels,)),
            pltpu.SemaphoreType.DMA,
            pltpu.SemaphoreType.DMA((levels - 1,)),
            pltpu.SemaphoreType.DMA((levels - 1,)),
            pltpu.SemaphoreType.DMA,
            pltpu.SemaphoreType.DMA,
        ],
        compiler_params=pltpu.CompilerParams(
            collective_id=0, has_side_effects=True, vmem_limit_bytes=60 * 1024 * 1024
        ),
    )(
        live_counts.reshape(1, levels),
        source_slot,
        target_owner,
        target_block,
        right_side.reshape(levels * slots * rhs, width),
        diag_inverse,
        off_blocks,
    )


def solution(mesh):
    sizes = tuple(mesh.shape[axis] for axis in AXES)
    in_specs = (
        P(None, AXES, None, None),
        P(None, AXES, None, None),
        P(None, AXES, None, None),
        P(None, AXES),
        P(None, AXES),
        P(None, AXES),
        P(None, AXES),
    )
    return jax.shard_map(
        functools.partial(shards, sizes),
        mesh=mesh,
        in_specs=in_specs,
        out_specs=P(None, AXES, None, None),
        check_vma=False,
    )
```

```python
import functools

import jax
import jax.numpy as jnp
from jax import lax
from jax.experimental import pallas as pl
from jax.experimental.pallas import tpu as pltpu
from jax.sharding import PartitionSpec as P

CAP = 2
GROUP = 4
AXES = ("gx", "gy", "gz")
MESH = pl.DeviceIdType.MESH


def kernel(
    sizes,
    live_ref,
    source_ref,
    owner_ref,
    block_ref,
    right_hbm,
    diag_hbm,
    off_hbm,
    out_hbm,
    work_ref,
    diag_ref,
    off_refs,
    solved_ref,
    outgoing_ref,
    arrived_ref,
    names_out_ref,
    names_ref,
    record_vmem,
    record_ref,
    load_sem,
    out_sem,
    record_sem,
    send_sem,
    recv_sem,
    name_send_sem,
    name_recv_sem,
):
    nx, ny, nz = sizes
    devices = nx * ny * nz
    plane = nx * nz
    levels, slots = diag_ref.shape[:2]
    records = off_refs[0].shape[0]
    rhs = solved_ref.shape[-2]
    pack = CAP * rhs
    level_rows = slots * rhs
    lanes = names_ref.shape[-1]
    mx, my, mz = (lax.axis_index(axis) for axis in AXES)
    me = (mx * ny + my) * nz + mz

    def partner(index):
        at = index // plane
        down = ny - 1 - at
        down = down - jnp.where(down > my, 0, 1)
        up = at + jnp.where(at < my, 0, 1)
        oy = jnp.where(at == ny - 1, my, jnp.where(2 * my < ny, down, up))
        rest = lax.rem(index, plane) + 1
        ox = lax.rem(mx + rest // nz, nx)
        oz = lax.rem(mz + lax.rem(rest, nz), nz)
        return (ox * ny + oy) * nz + oz, (ox, oy, oz)

    right_load = pltpu.make_async_copy(right_hbm, work_ref, load_sem.at[0])
    diag_loads = [
        pltpu.make_async_copy(diag_hbm.at[at], diag_ref.at[at], load_sem.at[1 + at])
        for at in range(levels)
    ]
    off_loads = [
        pltpu.make_async_copy(off_hbm.at[at], off_refs[at], load_sem.at[1 + levels + at])
        for at in range(levels - 1)
    ]
    barrier = pltpu.get_barrier_semaphore()

    @pl.loop(0, devices - 1)
    def _(index):
        pl.semaphore_signal(barrier, inc=1, device_id=partner(index)[1], device_id_type=MESH)

    right_load.start()
    for at in range(levels):
        diag_loads[at].start()
        if at < levels - 1:
            off_loads[at].start()

    owner_ids = lax.broadcasted_iota(jnp.int32, (devices, records), 0)
    record_ids = lax.broadcasted_iota(jnp.int32, (devices, records), 1)
    lane_ids = lax.broadcasted_iota(jnp.int32, (devices, lanes), 1)
    told = jnp.zeros((devices, lanes), jnp.float32)
    index = jnp.zeros((devices, lanes), jnp.int32)
    for at in range(levels - 1):
        hits = owner_ids == owner_ref[at : at + 1, :]
        block_row = (block_ref[at : at + 1, :] + 1).astype(jnp.float32)
        first = jnp.min(jnp.where(hits, record_ids, records - 1), axis=1, keepdims=True)
        last = jnp.max(jnp.where(hits, record_ids, 0), axis=1, keepdims=True)
        for copy_at, record in enumerate((first, last)):
            chosen = jnp.where(hits & (record_ids == record), block_row, 0.0)
            label = jnp.sum(chosen, axis=1, keepdims=True)
            told = jnp.where(lane_ids == at * CAP + copy_at, label, told)
            index = jnp.where(lane_ids == at * CAP + copy_at, record, index)
    record_vmem[...] = index
    names_out_ref[...] = told.reshape(devices, 1, lanes)
    names_ref[pl.ds(me, 1)] = names_out_ref[pl.ds(me, 1)]
    record_copy = pltpu.make_async_copy(record_vmem, record_ref, record_sem)
    record_copy.start()

    def solve(at):
        diag_loads[at].wait()
        count = live_ref[0, at]
        for slot in range(slots):
            row = (at * slots + slot) * rhs
            work = work_ref[row : row + rhs, :].astype(jnp.bfloat16)
            solved = jnp.dot(work, diag_ref[at, slot], preferred_element_type=jnp.float32)
            solved_ref[at, slot] = jnp.where(slot < count, solved, jnp.float32(0.0))
        pltpu.make_async_copy(solved_ref.at[at], out_hbm.at[at], out_sem.at[at]).start()

    def make(at, other, target_ref, base):
        for copy_at in range(CAP):
            record = record_ref[other, at * CAP + copy_at]
            picked = solved_ref[at, source_ref[at, record]].astype(jnp.bfloat16)
            target_ref[at, pl.ds(base + copy_at * rhs, rhs), :] = jnp.dot(
                picked, off_refs[at][record], preferred_element_type=jnp.float32
            )

    def make_out(at, index):
        other, _ = partner(index)
        make(at, other, outgoing_ref, other * pack)

    def send(at, index):
        other, where = partner(index)
        pltpu.make_async_remote_copy(
            src_ref=outgoing_ref.at[at, pl.ds(other * pack, pack)],
            dst_ref=arrived_ref.at[at, pl.ds(me * pack, pack)],
            send_sem=send_sem.at[at],
            recv_sem=recv_sem.at[at],
            device_id=where,
            device_id_type=MESH,
        ).start()

    def send_all(at):
        groups = devices // GROUP

        @pl.loop(0, groups - 1)
        def _(group):
            for item in range(GROUP):
                make_out(at, group * GROUP + item)
            for item in range(GROUP):
                send(at, group * GROUP + item)

        for index in range(devices - GROUP, devices - 1):
            make_out(at, index)
        for index in range(devices - GROUP, devices - 1):
            send(at, index)
        make(at, me, arrived_ref, me * pack)

    def gather_in(at, names, first, count):
        ids = lax.broadcasted_iota(jnp.int32, (count * slots, devices), 0) + (first * slots + 1)
        hits = [
            (ids == names[at * CAP + copy_at : at * CAP + copy_at + 1, :])
            .astype(jnp.float32)
            .astype(jnp.bfloat16)
            for copy_at in range(CAP)
        ]
        placer = jnp.concatenate(hits + hits, axis=1)
        for r in range(rhs):
            rows = [
                arrived_ref[at, pl.ds(copy_at * rhs + r, devices, stride=pack), :]
                for copy_at in range(CAP)
            ]
            high = [row.astype(jnp.bfloat16) for row in rows]
            low = [
                (row - top.astype(jnp.float32)).astype(jnp.bfloat16)
                for row, top in zip(rows, high)
            ]
            total = jnp.dot(
                placer,
                jnp.concatenate(high + low, axis=0),
                preferred_element_type=jnp.float32,
            )
            where = pl.ds(first * level_rows + r, count * slots, stride=rhs)
            work_ref[where, :] = work_ref[where, :] - total

    right_load.wait()
    solve(0)
    record_copy.wait()
    off_loads[0].wait()
    pl.semaphore_wait(barrier, devices - 1)

    @pl.loop(0, devices - 1)
    def _(index):
        other, where = partner(index)
        pltpu.make_async_remote_copy(
            src_ref=names_out_ref.at[pl.ds(other, 1)],
            dst_ref=names_ref.at[pl.ds(me, 1)],
            send_sem=name_send_sem,
            recv_sem=name_recv_sem,
            device_id=where,
            device_id_type=MESH,
        ).start()

    send_all(0)
    name_part = names_ref.at[pl.ds(0, devices - 1)]
    pltpu.make_async_copy(name_part, name_part, name_recv_sem).wait()
    wanted = -(-(levels - 1) * CAP // 8) * 8
    pick = (
        lax.broadcasted_iota(jnp.int32, (wanted, lanes), 0)
        == lax.broadcasted_iota(jnp.int32, (wanted, lanes), 1)
    ).astype(jnp.float32)
    names = lax.dot_general(
        pick,
        names_ref[...].reshape(devices, lanes),
        (((1,), (1,)), ((), ())),
        preferred_element_type=jnp.float32,
        precision=lax.Precision.HIGHEST,
    ).astype(jnp.int32)

    for at in range(1, levels):
        incoming = arrived_ref.at[at - 1, pl.ds(0, (devices - 1) * pack)]
        pltpu.make_async_copy(incoming, incoming, recv_sem.at[at - 1]).wait()
        gather_in(at - 1, names, at, 1)
        solve(at)
        if at < levels - 1:
            off_loads[at].wait()
            send_all(at)
            gather_in(at - 1, names, at + 1, levels - 1 - at)

    for at in range(levels):
        pltpu.make_async_copy(solved_ref.at[at], out_hbm.at[at], out_sem.at[at]).wait()
    name_part = names_out_ref.at[pl.ds(0, devices - 1)]
    pltpu.make_async_copy(name_part, name_part, name_send_sem).wait()
    for at in range(levels - 1):
        part = outgoing_ref.at[at, pl.ds(0, (devices - 1) * pack)]
        pltpu.make_async_copy(part, part, send_sem.at[at]).wait()


def shards(
    sizes,
    right_side,
    diag_inverse,
    off_blocks,
    live_counts,
    source_slot,
    target_owner,
    target_block,
):
    levels, slots, rhs, width = right_side.shape
    records = off_blocks.shape[1]
    devices = sizes[0] * sizes[1] * sizes[2]
    arrivals = devices * CAP
    lanes = 128
    smem = pl.BlockSpec(memory_space=pltpu.SMEM)
    vmem = pl.BlockSpec(memory_space=pltpu.VMEM)
    anywhere = pl.BlockSpec(memory_space=pl.ANY)
    return pl.pallas_call(
        functools.partial(kernel, sizes),
        out_shape=jax.ShapeDtypeStruct((levels, slots, rhs, width), jnp.float32),
        in_specs=[smem, smem, vmem, vmem, anywhere, anywhere, anywhere],
        out_specs=anywhere,
        scratch_shapes=[
            pltpu.VMEM((levels * slots * rhs, width), jnp.float32),
            pltpu.VMEM(diag_inverse.shape, diag_inverse.dtype),
            tuple(
                pltpu.VMEM(off_blocks.shape[1:], off_blocks.dtype) for _ in range(levels - 1)
            ),
            pltpu.VMEM((levels, slots, rhs, width), jnp.float32),
            pltpu.VMEM((levels - 1, arrivals * rhs, width), jnp.float32),
            pltpu.VMEM((levels - 1, arrivals * rhs, width), jnp.float32),
            pltpu.VMEM((devices, 1, lanes), jnp.float32),
            pltpu.VMEM((devices, 1, lanes), jnp.float32),
            pltpu.VMEM((devices, lanes), jnp.int32),
            pltpu.SMEM((devices, lanes), jnp.int32),
            pltpu.SemaphoreType.DMA((2 * levels,)),
            pltpu.SemaphoreType.DMA((levels,)),
            pltpu.SemaphoreType.DMA,
            pltpu.SemaphoreType.DMA((levels - 1,)),
            pltpu.SemaphoreType.DMA((levels - 1,)),
            pltpu.SemaphoreType.DMA,
            pltpu.SemaphoreType.DMA,
        ],
        compiler_params=pltpu.CompilerParams(
            collective_id=0, has_side_effects=True, vmem_limit_bytes=60 * 1024 * 1024
        ),
    )(
        live_counts.reshape(1, levels),
        source_slot,
        target_owner,
        target_block,
        right_side.reshape(levels * slots * rhs, width),
        diag_inverse,
        off_blocks,
    )


def solution(mesh):
    sizes = tuple(mesh.shape[axis] for axis in AXES)
    in_specs = (
        P(None, AXES, None, None),
        P(None, AXES, None, None),
        P(None, AXES, None, None),
        P(None, AXES),
        P(None, AXES),
        P(None, AXES),
        P(None, AXES),
    )
    return jax.shard_map(
        functools.partial(shards, sizes),
        mesh=mesh,
        in_specs=in_specs,
        out_specs=P(None, AXES, None, None),
        check_vma=False,
    )
```
